32 devices in a mesh: mem: 4 (over x, core), tile: 8 (over z, y).
Axes of the slice: x: 2, y: 2, z: 4, core: 2. Of those that a mesh axis runs over, the one named last changes fastest.
Arguments:
- alpha: bfloat16 [80, 64, 32, 128], P('mem', 'tile'), may hold values from -0.8984375 to 0.8984375
- ensemble: bfloat16 [80, 3, 64, 32, 128], P('mem', None, 'tile'), may hold values from -6 to 6
- loc_vert: bfloat16 [128, 128], replicated, may hold values from -0.25 to 1.5, as said below
- obs_col: int32 [8, 2048], P('tile'), may hold values from 0 to 1023
- obs_lev: int32 [8, 2048], P('tile'), may hold values from 0 to 127
- obs_count: int32 [8], P('tile'), may hold values from 512 to 2048
- innovation: float32 [8, 2048], P('tile'), may hold values from -6 to 6
- obs_weight: float32 [8, 2048], P('tile'), may hold values from 1 to 8
Outputs:
- gradient: float32 [80, 64, 32, 128], P('mem', 'tile')
The draws below stay inside these ranges and needn't reach their ends.
Inputs may be any that keep to these rules, and one draw needn't show every extreme that they name: `loc_vert`: a square root of the vertical localization, applied along levels.
All inputs are finite; a program needn't handle non-finite values.
Results may differ from the reference program's by a relative error of at most 0.0019.
Values sent between devices are 32-bit elements; how exact they have to be, the bound alone decides.
A program may use at most 64 MiB of HBM per device.

```python
import math
import jax
import jax.numpy as jnp
from jax import lax

V = 3
L = 128
NS = 2
CY = 8
CX = 32
NOBS = 2048
MEMBERS = 80
NYC = 64
TILES = 8


def draw_loc_vert(key, part):
    base = jax.random.fold_in(key, 11)
    first, second = jax.random.split(base)
    diagonal = jax.random.uniform(first, (L,), jnp.float32, 0.5, 1.5)
    others = jax.random.normal(second, (L, L), jnp.float32) * (0.5 / jnp.sqrt(L * 1.0))
    whole = jnp.eye(L, dtype=jnp.float32) * diagonal[None, :] + others
    whole = jnp.clip(whole, -0.25, 1.5)
    return whole.astype(jnp.bfloat16)


def plant(array, key, smallest, high):
    longest = array.shape.index(max(array.shape))
    spots = []
    for shift in (0, 1):
        where = [jax.random.randint(jax.random.fold_in(key, axis), (), 0, length) for axis, length in enumerate(array.shape)]
        where[longest] = (where[longest] + shift) % array.shape[longest]
        spots.append(tuple(where))
    return array.at[spots[0]].set(smallest).at[spots[1]].set(high)


def block_scale(key, extent, pieces, smallest, high):
    def one(position, parts):
        draws = jax.random.uniform(jax.random.fold_in(jax.random.fold_in(key, 6), position), (parts,), jnp.float32, smallest / len(pieces), high / len(pieces))
        return jnp.repeat(jnp.exp(draws), extent[position] // parts).reshape((-1,) + (1,) * (len(extent) - position - 1))

    level = one(*pieces[0])
    for cut in pieces[1:]:
        level = level * one(*cut)
    return level


def normal_values(own_key, shape, width, reach, shards=(), kind=jnp.bfloat16):
    gain = block_scale(own_key, shape, shards, -0.22, 0.18) if shards else 1.0
    drawn = jax.random.normal(own_key, shape, jnp.float32) * width * gain
    return jnp.minimum(jnp.maximum(drawn, -reach), reach).astype(kind)


def setup_inputs(seed: int = 0) -> dict:
    key_of = jax.random.split(jax.random.key(seed), 9)
    alpha = normal_values(key_of[0], (MEMBERS, NYC, CX, L), 0.15, 0.8984375, ((0, 4), (1, 8)))
    ensemble = normal_values(key_of[1], (MEMBERS, V, NYC, CX, L), 1.0, 6.0, ((0, 4), (2, 8)))
    loc_vert = draw_loc_vert(jax.random.fold_in(key_of[8], 71), 0)
    obs_col = plant(jax.random.randint(key_of[3], (TILES, NOBS), 0, 4 * CY * CX), jax.random.fold_in(key_of[3], 1), 0, (4 * CY * CX) - 1).astype(jnp.int32)
    obs_lev = plant(jax.random.randint(key_of[4], (TILES, NOBS), 0, L), jax.random.fold_in(key_of[4], 1), 0, L - 1).astype(jnp.int32)
    obs_count = plant(jax.random.randint(key_of[5], (TILES,), NOBS // 4, NOBS + 1), jax.random.fold_in(key_of[5], 1), NOBS // 4, NOBS).astype(jnp.int32)
    innovation = normal_values(key_of[6], (TILES, NOBS), 1.0, 6.0, ((0, 8),), jnp.float32)
    obs_weight = jnp.clip(jnp.exp(math.log(8.0) - 2.0794415 * jax.random.uniform(key_of[7], (TILES, NOBS), jnp.float32) ** block_scale(key_of[7], (TILES, NOBS), ((0, 8),), -0.2, 0.2)), 1.0, 8.0)
    return dict(alpha=alpha, ensemble=ensemble, loc_vert=loc_vert, obs_col=obs_col, obs_lev=obs_lev, obs_count=obs_count, innovation=innovation, obs_weight=obs_weight)


def widen(field, axis):
    pads = [(1, 1) if dim == axis else (0, 0) for dim in range(field.ndim)]
    return jnp.pad(field, pads)


def spread(padded, axis):
    length = padded.shape[axis] - 2
    before = lax.slice_in_dim(padded, 0, length, axis=axis)
    middle = lax.slice_in_dim(padded, 1, length + 1, axis=axis)
    after = lax.slice_in_dim(padded, 2, length + 2, axis=axis)
    return 0.25 * before + 0.5 * middle + 0.25 * after


def smooth(field, row_axis):
    for sweep in range(NS):
        field = spread(widen(field, row_axis), row_axis)
        field = spread(widen(field, row_axis + 1), row_axis + 1)
    return field


def refine(padded, axis):
    length = padded.shape[axis] - 2
    before = lax.slice_in_dim(padded, 0, length, axis=axis)
    middle = lax.slice_in_dim(padded, 1, length + 1, axis=axis)
    after = lax.slice_in_dim(padded, 2, length + 2, axis=axis)
    evens = 0.75 * middle + 0.25 * before
    odds = 0.75 * middle + 0.25 * after
    stacked = jnp.stack([evens, odds], axis=axis + 1)
    shape = list(middle.shape)
    shape[axis] = 2 * length
    return stacked.reshape(shape)


def coarsen(padded, axis):
    length = padded.shape[axis] - 2
    first = lax.slice_in_dim(padded, 0, length, 2, axis=axis)
    second = lax.slice_in_dim(padded, 1, length + 1, 2, axis=axis)
    third = lax.slice_in_dim(padded, 2, length + 2, 2, axis=axis)
    fourth = lax.slice_in_dim(padded, 3, length + 2, 2, axis=axis)
    return 0.25 * first + 0.75 * second + 0.75 * third + 0.25 * fourth


def reference(alpha, ensemble, loc_vert, obs_col, obs_lev, obs_count, innovation, obs_weight):
    def add_member(running, member_item):
        control, member = member_item
        lifted = smooth(jnp.dot(control, loc_vert.T, preferred_element_type=jnp.float32), 0).astype(jnp.bfloat16)
        return running + member.astype(jnp.float32) * lifted.astype(jnp.float32)[None], 0

    initial = jnp.zeros(ensemble.shape[1:], jnp.float32)
    increment, unused = lax.scan(add_member, initial, (alpha, ensemble))
    fine = refine(widen(refine(widen(increment, 1), 1), 2), 2)
    strips = obs_col.shape[0]
    slots = obs_col.shape[1]
    strip_rows = fine.shape[1] // strips
    fine_width = fine.shape[2]
    variable = jnp.broadcast_to((jnp.arange(slots, dtype=jnp.int32) % V)[None, :], (strips, slots))
    row_index = jnp.arange(strips, dtype=jnp.int32)[:, None] * strip_rows + obs_col // fine_width
    col_index = obs_col % fine_width
    values = fine[variable, row_index, col_index, obs_lev]
    live = jnp.arange(slots, dtype=jnp.int32)[None, :] < obs_count[:, None]
    weighted = jnp.where(live, obs_weight * (values - innovation), jnp.zeros_like(values))
    fine_adjoint = jnp.zeros_like(fine).at[variable, row_index, col_index, obs_lev].add(weighted)
    coarse_adjoint = coarsen(widen(coarsen(widen(fine_adjoint, 2), 2), 1), 1)

    def member_gradient(member_item):
        control, member = member_item
        back = jnp.sum(member.astype(jnp.float32) * coarse_adjoint, axis=0)
        back = smooth(back, 0)
        return control.astype(jnp.float32) + jnp.dot(back, loc_vert.astype(jnp.float32), precision=lax.Precision.HIGHEST)

    return lax.map(member_gradient, (alpha, ensemble))
```

```python
import functools

import jax
import jax.numpy as jnp
from jax import lax
from jax.experimental import pallas as pl
from jax.experimental.pallas import tpu as pltpu
from jax.sharding import PartitionSpec as P

V = 3
F32 = jnp.float32
BF16 = jnp.bfloat16
MESH = pl.DeviceIdType.MESH


def split2(x):
    hi = x.astype(BF16)
    lo = (x - hi.astype(F32)).astype(BF16)
    return hi, lo


def dot(a, b):
    return jnp.dot(a, b, preferred_element_type=F32)


def dot_nt(a, b):
    return lax.dot_general(a, b, (((1,), (1,)), ((), ())), preferred_element_type=F32)


def band(distance):
    d = jnp.abs(distance)
    return jnp.where(d == 0, 6.0, jnp.where(d == 1, 4.0, jnp.where(d == 2, 1.0, 0.0)))


def column_weight(c, c2, cols):
    end = (c == c2) & ((c == 0) | (c == cols - 1))
    return (band(c - c2) - jnp.where(end, 1.0, 0.0)) * (1.0 / 16.0)


def kernel(n, tiles, chunks, alpha, ens_hbm, loc, col, lev, cnt, innov, wgt, out,
           ens, hs, hr, gs, gr, lbe, mm, em, wt, inci, ince, reci, rece, redi, rede,
           incf, incg, ihalo, adj, adjs, ahalo,
           ens_sem, hs_sem, hr_sem, gs_sem, gr_sem, rs_s, rs_r, ag_s, ag_r, ih_s, ih_r, ah_s, ah_r):
    members, rows, cols, levels = alpha.shape
    size = rows * cols
    cq = cols // n
    per = members // chunks
    m = lax.axis_index("mem")
    t = lax.axis_index("tile")
    has = (t > 0, t < tiles - 1)
    near = (t - 1, t + 1)
    ens_copy = pltpu.make_async_copy(ens_hbm, ens, ens_sem)
    ens_copy.start()

    barrier = pltpu.get_barrier_semaphore()
    for d in range(1, n):
        pl.semaphore_signal(barrier, inc=1, device_id={"mem": lax.rem(m + d, n), "tile": t}, device_id_type=MESH)
    for s in range(2):
        @pl.when(has[s])
        def _(s=s):
            pl.semaphore_signal(barrier, inc=1, device_id={"mem": m, "tile": near[s]}, device_id_type=MESH)

    hs[0] = alpha[:, 0:2].astype(F32)
    hs[1] = alpha[:, rows - 2 : rows].astype(F32)
    pl.semaphore_wait(barrier, n - 1 + has[0].astype(jnp.int32) + has[1].astype(jnp.int32))

    def halo(src, dst, ssem, rsem, s):
        return pltpu.make_async_remote_copy(
            src_ref=src, dst_ref=dst, send_sem=ssem, recv_sem=rsem,
            device_id={"mem": m, "tile": near[s]}, device_id_type=MESH)

    def edge_copy(src, dst, ssem, rsem, s, c):
        part = pl.ds(c * per, per)
        return halo(src.at[s, part], dst.at[1 - s, part], ssem.at[s, c], rsem.at[1 - s, c], s)

    for c in range(chunks):
        for s in range(2):
            @pl.when(has[s])
            def _(s=s, c=c):
                edge_copy(hs, hr, hs_sem, hr_sem, s, c).start()
    for s in range(2):
        @pl.when(jnp.logical_not(has[s]))
        def _(s=s):
            hr[s] = jnp.zeros(hr.shape[1:], F32)
            gr[s] = jnp.zeros(gr.shape[1:], F32)
            ihalo[s] = jnp.zeros(ihalo.shape[1:], F32)
            ahalo[s] = jnp.zeros(ahalo.shape[1:], F32)

    i = lax.broadcasted_iota(jnp.int32, (size, size), 0)
    j = lax.broadcasted_iota(jnp.int32, (size, size), 1)
    r, r2 = lax.div(i, cols), lax.div(j, cols)
    end = (r == r2) & (((r == 0) & (t == 0)) | ((r == rows - 1) & (t == tiles - 1)))
    row_weight = (band(r - r2) - jnp.where(end, 1.0, 0.0)) * (1.0 / 16.0)
    mm[...] = (row_weight * column_weight(i - r * cols, j - r2 * cols, cols)).astype(BF16)
    i = lax.broadcasted_iota(jnp.int32, (4 * cols, 4 * cols), 0)
    j = lax.broadcasted_iota(jnp.int32, (4 * cols, 4 * cols), 1)
    q, q2 = lax.div(i, cols), lax.div(j, cols)
    r = jnp.where(q < 2, q, q + rows - 4)
    r2 = jnp.where(q2 < 2, q2 - 2, q2 - 2 + rows)
    em[...] = (band(r - r2) * (1.0 / 16.0) * column_weight(i - q * cols, j - q2 * cols, cols)).astype(BF16)

    inci[...] = jnp.zeros_like(inci)
    ince[...] = jnp.zeros_like(ince)
    ens_copy.wait()
    lv = loc[...]

    def lift(k, carry):
        hi, lo = split2(dot(mm[...], alpha[k].reshape(size, levels)))
        base = (dot_nt(hi, lv) + dot_nt(lo, lv)).reshape(rows, cols, levels)
        lbe[k, 0:2] = base[0:2]
        lbe[k, 2:4] = base[rows - 2 : rows]
        inner = base[2 : rows - 2].astype(BF16).astype(F32)
        for v in range(V):
            inci[v] += ens[k, v, 2 : rows - 2].astype(F32) * inner
        return carry

    lax.fori_loop(0, members, lift, 0)

    def spread_copy(part, rec, d, which):
        peer = lax.rem(m + d, n)
        return pltpu.make_async_remote_copy(
            src_ref=part.at[:, :, pl.ds(pl.multiple_of(peer * cq, cq), cq), :], dst_ref=rec.at[d - 1],
            send_sem=rs_s.at[which, d - 1], recv_sem=rs_r.at[which, d - 1],
            device_id={"mem": peer, "tile": t}, device_id_type=MESH)

    def gather_copy(red, full, d, which):
        peer = lax.rem(m + d, n)
        return pltpu.make_async_remote_copy(
            src_ref=red, dst_ref=full.at[:, :, pl.ds(pl.multiple_of(m * cq, cq), cq), :],
            send_sem=ag_s.at[which, d - 1], recv_sem=ag_r.at[which, d - 1],
            device_id={"mem": peer, "tile": t}, device_id_type=MESH)

    def reduce(part, rec, red, full, which):
        mine = pl.ds(pl.multiple_of(m * cq, cq), cq)
        for d in range(1, n):
            spread_copy(part, rec, d, which).start()
        total = part[:, :, mine, :]
        for d in range(1, n):
            spread_copy(part, rec, d, which).wait_recv()
            total = total + rec[d - 1]
        red[...] = total
        for d in range(1, n):
            gather_copy(red, full, d, which).start()
        full[:, :, mine, :] = total

    def finish(part, rec, red, full, which):
        for d in range(1, n):
            gather_copy(red, full, d, which).wait_recv()
        for d in range(1, n):
            spread_copy(part, rec, d, which).wait_send()
            gather_copy(red, full, d, which).wait_send()

    reduce(inci, reci, redi, incf, 0)

    slots = col.shape[1]
    place = col[...]
    wide = 2 * cols
    frow = lax.div(place, wide)
    fcol = place - frow * wide
    slot = lax.broadcasted_iota(jnp.int32, (1, slots), 1)
    variable = lax.rem(slot, V)

    def weights(fine, count, shift):
        main = lax.div(fine, 2)
        other = jnp.where(fine - 2 * main == 1, main + 1, main - 1)
        at = lax.broadcasted_iota(jnp.int32, (count, slots), 0) - shift
        return jnp.where(at == main, 0.75, 0.0) + jnp.where(at == other, 0.25, 0.0)

    wr = weights(frow, rows + 2, 1)
    wc = weights(fcol, cols, 0)
    for v in range(V):
        mask = jnp.where(variable == v, 1.0, 0.0)
        for a in range(rows + 2):
            start = (v * (rows + 2) + a) * cols
            wt[start : start + cols, :] = (wc * (wr[a : a + 1, :] * mask)).astype(BF16)
    finish(inci, reci, redi, incf, 0)

    for c in range(chunks):
        for s in range(2):
            @pl.when(has[s])
            def _(s=s, c=c):
                part = pl.ds(c * per, per)
                halo(hs.at[s, part], hr.at[s, part], hs_sem.at[s, c], hr_sem.at[s, c], s).wait_recv()

        def lift_edge(k, carry):
            around = jnp.concatenate([hr[0, k], hr[1, k]], axis=0).astype(BF16).reshape(4 * cols, levels)
            hi, lo = split2(dot(em[...], around))
            edge = (dot_nt(hi, lv) + dot_nt(lo, lv)).reshape(4, cols, levels) + lbe[k]
            edge = edge.astype(BF16).astype(F32)
            for v in range(V):
                ince[v, 0:2] += ens[k, v, 0:2].astype(F32) * edge[0:2]
                ince[v, 2:4] += ens[k, v, rows - 2 : rows].astype(F32) * edge[2:4]
            return carry

        lax.fori_loop(c * per, (c + 1) * per, lift_edge, 0)

    reduce(ince, rece, rede, incg, 1)
    finish(ince, rece, rede, incg, 1)

    def ihalo_copy(s):
        return halo(incg.at[:, 3 * s], ihalo.at[1 - s], ih_s.at[s], ih_r.at[1 - s], s)

    def ihalo_wait(s):
        return halo(incg.at[:, 3 * s], ihalo.at[s], ih_s.at[s], ih_r.at[s], s)

    for s in range(2):
        @pl.when(has[s])
        def _(s=s):
            ihalo_copy(s).start()
    for s in range(2):
        @pl.when(has[s])
        def _(s=s):
            ihalo_wait(s).wait_recv()
            ihalo_copy(s).wait_send()

    places = V * (rows + 2) * cols
    whole = jnp.concatenate(
        [ihalo[0][:, None], incg[:, 0:2], incf[...], incg[:, 2:4], ihalo[1][:, None]], axis=1
    ).reshape(places, levels)
    flipped = whole.T
    hi, lo = split2(flipped)
    picked = dot(hi, wt[...]) + dot(lo, wt[...])
    hot = lax.broadcasted_iota(jnp.int32, (levels, slots), 0) == lev[...]
    value = jnp.sum(jnp.where(hot, picked, 0.0), axis=0, keepdims=True)
    weighted = jnp.where(slot < cnt[0], wgt[...] * (value - innov[...]), 0.0)
    sent = jnp.where(hot, jnp.broadcast_to(weighted, hot.shape), 0.0)
    hi, lo = split2(sent)
    adjoint = (dot_nt(wt[...], hi) + dot_nt(wt[...], lo)).reshape(V, rows + 2, cols, levels)
    adjs[0] = adjoint[:, 0]
    adjs[1] = adjoint[:, rows + 1]

    def ahalo_copy(s, slot_there):
        return halo(adjs.at[s], ahalo.at[slot_there], ah_s.at[s], ah_r.at[slot_there], s)

    for s in range(2):
        @pl.when(has[s])
        def _(s=s):
            ahalo_copy(s, 1 - s).start()
    adj[...] = adjoint[:, 1 : rows + 1]
    for s in range(2):
        @pl.when(has[s])
        def _(s=s):
            ahalo_copy(s, s).wait_recv()
            ahalo_copy(s, 1 - s).wait_send()
    adj[:, 0] += ahalo[0]
    adj[:, rows - 1] += ahalo[1]

    def field(k, low, high):
        total = ens[k, 0, low:high].astype(F32) * adj[0, low:high]
        for v in range(1, V):
            total = total + ens[k, v, low:high].astype(F32) * adj[v, low:high]
        return total

    for c in range(chunks):
        def edges(k, carry):
            gs[0, k] = field(k, 0, 2)
            gs[1, k] = field(k, rows - 2, rows)
            return carry

        lax.fori_loop(c * per, (c + 1) * per, edges, 0)
        for s in range(2):
            @pl.when(has[s])
            def _(s=s, c=c):
                edge_copy(gs, gr, gs_sem, gr_sem, s, c).start()

    def raised(x):
        hi, lo = split2(x)
        return split2(dot(hi, lv) + dot(lo, lv))

    def inside(k, carry):
        g = jnp.concatenate([gs[0, k], field(k, 2, rows - 2), gs[1, k]], axis=0).reshape(size, levels)
        hi, lo = raised(g)
        back = dot(mm[...], hi) + dot(mm[...], lo)
        out[k] = alpha[k].astype(F32) + back.reshape(rows, cols, levels)
        return carry

    lax.fori_loop(0, members, inside, 0)

    for c in range(chunks):
        for s in range(2):
            @pl.when(has[s])
            def _(s=s, c=c):
                part = pl.ds(c * per, per)
                halo(gs.at[s, part], gr.at[s, part], gs_sem.at[s, c], gr_sem.at[s, c], s).wait_recv()

        def outer(k, carry):
            around = jnp.concatenate([gr[0, k], gr[1, k]], axis=0).reshape(4 * cols, levels)
            hi, lo = raised(around)
            back = (dot(em[...], hi) + dot(em[...], lo)).reshape(4, cols, levels)
            out[k, 0:2] += back[0:2]
            out[k, rows - 2 : rows] += back[2:4]
            return carry

        lax.fori_loop(c * per, (c + 1) * per, outer, 0)
    for c in range(chunks):
        for s in range(2):
            @pl.when(has[s])
            def _(s=s, c=c):
                edge_copy(hs, hr, hs_sem, hr_sem, s, c).wait_send()
                edge_copy(gs, gr, gs_sem, gr_sem, s, c).wait_send()


def solution(mesh):
    n = mesh.shape["mem"]
    tiles = mesh.shape["tile"]

    def on_device(alpha, ensemble, loc_vert, obs_col, obs_lev, obs_count, innovation, obs_weight):
        members, rows, cols, levels = alpha.shape
        slots = obs_col.shape[1]
        chunks = 4 if members % 4 == 0 else 1
        cq = cols // n
        vmem = pl.BlockSpec(memory_space=pltpu.VMEM)
        edge = pltpu.VMEM((2, members, 2, cols, levels), F32)
        dma = pltpu.SemaphoreType.DMA
        return pl.pallas_call(
            functools.partial(kernel, n, tiles, chunks),
            out_shape=jax.ShapeDtypeStruct(alpha.shape, F32),
            in_specs=[vmem, pl.BlockSpec(memory_space=pl.ANY), vmem, vmem, vmem,
                      pl.BlockSpec(memory_space=pltpu.SMEM), vmem, vmem],
            out_specs=vmem,
            scratch_shapes=[
                pltpu.VMEM(ensemble.shape, BF16), edge, edge, edge, edge,
                pltpu.VMEM((members, 4, cols, levels), F32),
                pltpu.VMEM((rows * cols, rows * cols), BF16),
                pltpu.VMEM((4 * cols, 4 * cols), BF16),
                pltpu.VMEM((V * (rows + 2) * cols, slots), BF16),
                pltpu.VMEM((V, rows - 4, cols, levels), F32),
                pltpu.VMEM((V, 4, cols, levels), F32),
                pltpu.VMEM((n - 1, V, rows - 4, cq, levels), F32),
                pltpu.VMEM((n - 1, V, 4, cq, levels), F32),
                pltpu.VMEM((V, rows - 4, cq, levels), F32),
                pltpu.VMEM((V, 4, cq, levels), F32),
                pltpu.VMEM((V, rows - 4, cols, levels), F32),
                pltpu.VMEM((V, 4, cols, levels), F32),
                pltpu.VMEM((2, V, cols, levels), F32),
                pltpu.VMEM((V, rows, cols, levels), F32),
                pltpu.VMEM((2, V, cols, levels), F32),
                pltpu.VMEM((2, V, cols, levels), F32),
                dma, dma((2, chunks)), dma((2, chunks)), dma((2, chunks)), dma((2, chunks)),
                dma((2, n - 1)), dma((2, n - 1)), dma((2, n - 1)), dma((2, n - 1)),
                dma((2,)), dma((2,)), dma((2,)), dma((2,)),
            ],
            compiler_params=pltpu.CompilerParams(
                collective_id=0, has_side_effects=True, vmem_limit_bytes=60 << 20),
        )(alpha, ensemble, loc_vert, obs_col, obs_lev, obs_count, innovation, obs_weight)

    in_specs = (
        P("mem", "tile", None, None),
        P("mem", None, "tile", None, None),
        P(),
        P("tile", None),
        P("tile", None),
        P("tile"),
        P("tile", None),
        P("tile", None),
    )
    out_specs = P("mem", "tile", None, None)
    return jax.shard_map(
        on_device, mesh=mesh, in_specs=in_specs, out_specs=out_specs, check_vma=False
    )
```

```python
import functools

import jax
import jax.numpy as jnp
from jax import lax
from jax.experimental import pallas as pl
from jax.experimental.pallas import tpu as pltpu
from jax.sharding import PartitionSpec as P

V = 3
F32 = jnp.float32
BF16 = jnp.bfloat16
MESH = pl.DeviceIdType.MESH


def split2(x):
    hi = x.astype(BF16)
    lo = (x - hi.astype(F32)).astype(BF16)
    return hi, lo


def dot(a, b):
    return jnp.dot(a, b, preferred_element_type=F32)


def dot_nt(a, b):
    return lax.dot_general(a, b, (((1,), (1,)), ((), ())), preferred_element_type=F32)


def band(distance):
    d = jnp.abs(distance)
    return jnp.where(d == 0, 6.0, jnp.where(d == 1, 4.0, jnp.where(d == 2, 1.0, 0.0)))


def column_weight(c, c2, cols):
    end = (c == c2) & ((c == 0) | (c == cols - 1))
    return (band(c - c2) - jnp.where(end, 1.0, 0.0)) * (1.0 / 16.0)


def kernel(n, tiles, chunks, alpha, ens_hbm, loc, col, lev, cnt, innov, wgt, out,
           ens, hs, hr, gs, gr, lbe, mm, em, wt, inci, ince, reci, rece, redi, rede,
           incf, incg, ihalo, adj, adjs, ahalo,
           ens_sem, hs_sem, hr_sem, gs_sem, gr_sem, rs_s, rs_r, ag_s, ag_r, ih_s, ih_r, ah_s, ah_r):
    members, rows, cols, levels = alpha.shape
    size = rows * cols
    cq = cols // n
    per = members // chunks
    m = lax.axis_index("mem")
    t = lax.axis_index("tile")
    has = (t > 0, t < tiles - 1)
    near = (t - 1, t + 1)
    ens_copy = pltpu.make_async_copy(ens_hbm, ens, ens_sem)
    ens_copy.start()

    barrier = pltpu.get_barrier_semaphore()
    for d in range(1, n):
        pl.semaphore_signal(barrier, inc=1, device_id={"mem": lax.rem(m + d, n), "tile": t}, device_id_type=MESH)
    for s in range(2):
        @pl.when(has[s])
        def _(s=s):
            for d in range(n):
                pl.semaphore_signal(barrier, inc=1, device_id={"mem": lax.rem(m + d, n), "tile": near[s]}, device_id_type=MESH)

    hs[0] = alpha[:, 0:2].astype(F32)
    hs[1] = alpha[:, rows - 2 : rows].astype(F32)
    pl.semaphore_wait(barrier, n - 1 + n * (has[0].astype(jnp.int32) + has[1].astype(jnp.int32)))

    def halo(src, dst, ssem, rsem, s):
        return pltpu.make_async_remote_copy(
            src_ref=src, dst_ref=dst, send_sem=ssem, recv_sem=rsem,
            device_id={"mem": m, "tile": near[s]}, device_id_type=MESH)

    def edge_copy(src, dst, ssem, rsem, s, c):
        part = pl.ds(c * per, per)
        return halo(src.at[s, part], dst.at[1 - s, part], ssem.at[s, c], rsem.at[1 - s, c], s)

    for c in range(chunks):
        for s in range(2):
            @pl.when(has[s])
            def _(s=s, c=c):
                edge_copy(hs, hr, hs_sem, hr_sem, s, c).start()
    for s in range(2):
        @pl.when(jnp.logical_not(has[s]))
        def _(s=s):
            hr[s] = jnp.zeros(hr.shape[1:], F32)
            gr[s] = jnp.zeros(gr.shape[1:], F32)
            ihalo[s] = jnp.zeros(ihalo.shape[1:], F32)
            ahalo[s] = jnp.zeros(ahalo.shape[1:], F32)

    i = lax.broadcasted_iota(jnp.int32, (size, size), 0)
    j = lax.broadcasted_iota(jnp.int32, (size, size), 1)
    r, r2 = lax.div(i, cols), lax.div(j, cols)
    end = (r == r2) & (((r == 0) & (t == 0)) | ((r == rows - 1) & (t == tiles - 1)))
    row_weight = (band(r - r2) - jnp.where(end, 1.0, 0.0)) * (1.0 / 16.0)
    mm[...] = (row_weight * column_weight(i - r * cols, j - r2 * cols, cols)).astype(BF16)
    i = lax.broadcasted_iota(jnp.int32, (4 * cols, 4 * cols), 0)
    j = lax.broadcasted_iota(jnp.int32, (4 * cols, 4 * cols), 1)
    q, q2 = lax.div(i, cols), lax.div(j, cols)
    r = jnp.where(q < 2, q, q + rows - 4)
    r2 = jnp.where(q2 < 2, q2 - 2, q2 - 2 + rows)
    em[...] = (band(r - r2) * (1.0 / 16.0) * column_weight(i - q * cols, j - q2 * cols, cols)).astype(BF16)

    inci[...] = jnp.zeros_like(inci)
    ince[...] = jnp.zeros_like(ince)
    ens_copy.wait()
    lv = loc[...]

    def lift(k, carry):
        hi, lo = split2(dot(mm[...], alpha[k].reshape(size, levels)))
        base = (dot_nt(hi, lv) + dot_nt(lo, lv)).reshape(rows, cols, levels)
        lbe[k, 0:2] = base[0:2]
        lbe[k, 2:4] = base[rows - 2 : rows]
        inner = base[2 : rows - 2].astype(BF16).astype(F32)
        for v in range(V):
            inci[v] += ens[k, v, 2 : rows - 2].astype(F32) * inner
        return carry

    lax.fori_loop(0, members, lift, 0)

    def spread_copy(part, rec, d, which):
        peer = lax.rem(m + d, n)
        return pltpu.make_async_remote_copy(
            src_ref=part.at[:, :, pl.ds(pl.multiple_of(peer * cq, cq), cq), :], dst_ref=rec.at[d - 1],
            send_sem=rs_s.at[which, d - 1], recv_sem=rs_r.at[which, d - 1],
            device_id={"mem": peer, "tile": t}, device_id_type=MESH)

    def gather_copy(red, full, d, which):
        peer = lax.rem(m + d, n)
        return pltpu.make_async_remote_copy(
            src_ref=red, dst_ref=full.at[:, :, pl.ds(pl.multiple_of(m * cq, cq), cq), :],
            send_sem=ag_s.at[which, d - 1], recv_sem=ag_r.at[which, d - 1],
            device_id={"mem": peer, "tile": t}, device_id_type=MESH)

    def ihalo_copy(s, slot, d):
        return pltpu.make_async_remote_copy(
            src_ref=rede.at[:, 3 * s], dst_ref=ihalo.at[slot, :, pl.ds(pl.multiple_of(m * cq, cq), cq), :],
            send_sem=ih_s.at[s, d], recv_sem=ih_r.at[slot, d],
            device_id={"mem": lax.rem(m + d, n), "tile": near[s]}, device_id_type=MESH)

    def reduce(part, rec, red, full, which):
        mine = pl.ds(pl.multiple_of(m * cq, cq), cq)
        for d in range(1, n):
            spread_copy(part, rec, d, which).start()
        total = part[:, :, mine, :]
        for d in range(1, n):
            spread_copy(part, rec, d, which).wait_recv()
            total = total + rec[d - 1]
        red[...] = total
        if which == 1:
            for s in range(2):
                @pl.when(has[s])
                def _(s=s):
                    for d in range(n):
                        ihalo_copy(s, 1 - s, d).start()
        for d in range(1, n):
            gather_copy(red, full, d, which).start()
        full[:, :, mine, :] = total

    def finish(part, rec, red, full, which):
        for d in range(1, n):
            gather_copy(red, full, d, which).wait_recv()
        for d in range(1, n):
            spread_copy(part, rec, d, which).wait_send()
            gather_copy(red, full, d, which).wait_send()

    reduce(inci, reci, redi, incf, 0)

    slots = col.shape[1]
    place = col[...]
    wide = 2 * cols
    frow = lax.div(place, wide)
    fcol = place - frow * wide
    slot = lax.broadcasted_iota(jnp.int32, (1, slots), 1)
    variable = lax.rem(slot, V)

    def weights(fine, count, shift):
        main = lax.div(fine, 2)
        other = jnp.where(fine - 2 * main == 1, main + 1, main - 1)
        at = lax.broadcasted_iota(jnp.int32, (count, slots), 0) - shift
        return jnp.where(at == main, 0.75, 0.0) + jnp.where(at == other, 0.25, 0.0)

    wr = weights(frow, rows + 2, 1)
    wc = weights(fcol, cols, 0)
    for v in range(V):
        mask = jnp.where(variable == v, 1.0, 0.0)
        for a in range(rows + 2):
            start = (a * V + v) * cols
            wt[start : start + cols, :] = (wc * (wr[a : a + 1, :] * mask)).astype(BF16)
    finish(inci, reci, redi, incf, 0)

    for c in range(chunks):
        for s in range(2):
            @pl.when(has[s])
            def _(s=s, c=c):
                part = pl.ds(c * per, per)
                halo(hs.at[s, part], hr.at[s, part], hs_sem.at[s, c], hr_sem.at[s, c], s).wait_recv()

        def lift_edge(k, carry):
            around = jnp.concatenate([hr[0, k], hr[1, k]], axis=0).astype(BF16).reshape(4 * cols, levels)
            hi, lo = split2(dot(em[...], around))
            edge = (dot_nt(hi, lv) + dot_nt(lo, lv)).reshape(4, cols, levels) + lbe[k]
            edge = edge.astype(BF16).astype(F32)
            for v in range(V):
                ince[v, 0:2] += ens[k, v, 0:2].astype(F32) * edge[0:2]
                ince[v, 2:4] += ens[k, v, rows - 2 : rows].astype(F32) * edge[2:4]
            return carry

        lax.fori_loop(c * per, (c + 1) * per, lift_edge, 0)

    reduce(ince, rece, rede, incg, 1)
    finish(ince, rece, rede, incg, 1)

    for s in range(2):
        @pl.when(has[s])
        def _(s=s):
            for d in range(n):
                ihalo_copy(s, s, d).wait_recv()
                ihalo_copy(s, 1 - s, d).wait_send()

    places = V * (rows + 2) * cols
    pieces = [ihalo[0], incg[:, 0], incg[:, 1]] + [incf[:, a] for a in range(rows - 4)]
    pieces += [incg[:, 2], incg[:, 3], ihalo[1]]
    whole = jnp.concatenate(pieces, axis=0).reshape(places, levels)
    flipped = whole.T
    hi, lo = split2(flipped)
    picked = dot(hi, wt[...]) + dot(lo, wt[...])
    hot = lax.broadcasted_iota(jnp.int32, (levels, slots), 0) == lev[...]
    value = jnp.sum(jnp.where(hot, picked, 0.0), axis=0, keepdims=True)
    weighted = jnp.where(slot < cnt[0], wgt[...] * (value - innov[...]), 0.0)
    sent = jnp.where(hot, jnp.broadcast_to(weighted, hot.shape), 0.0)
    hi, lo = split2(sent)
    sent2 = jnp.concatenate([hi, lo], axis=0)

    def adjoint(a, count):
        both = dot_nt(wt[a * V * cols : (a + count) * V * cols, :], sent2)
        return (both[:, :levels] + both[:, levels:]).reshape(count, V, cols, levels)

    adjs[0] = adjoint(0, 1)[0]
    adjs[1] = adjoint(rows + 1, 1)[0]

    def ahalo_copy(s, slot_there):
        return halo(adjs.at[s], ahalo.at[slot_there], ah_s.at[s], ah_r.at[slot_there], s)

    for s in range(2):
        @pl.when(has[s])
        def _(s=s):
            ahalo_copy(s, 1 - s).start()
    top, bottom = adjoint(1, 2), adjoint(rows - 1, 2)
    for a in range(2):
        adj[:, a] = top[a]
        adj[:, rows - 2 + a] = bottom[a]

    def field(k, low, high):
        total = ens[k, 0, low:high].astype(F32) * adj[0, low:high]
        for v in range(1, V):
            total = total + ens[k, v, low:high].astype(F32) * adj[v, low:high]
        return total

    def back_copy(s, slot, w, c):
        part = pl.ds(c * per, per)
        return halo(gs.at[s, w, part], gr.at[slot, w, part], gs_sem.at[s, w, c], gr_sem.at[slot, w, c], s)

    def send_row(w):
        where = (1 - w, rows - 2 + w)
        for c in range(chunks):
            def edges(k, carry):
                for s in range(2):
                    gs[s, w, k] = field(k, where[s], where[s] + 1)[0]
                return carry

            lax.fori_loop(c * per, (c + 1) * per, edges, 0)
            for s in range(2):
                @pl.when(has[s])
                def _(s=s, c=c):
                    back_copy(s, 1 - s, w, c).start()

    send_row(0)
    for s in range(2):
        @pl.when(has[s])
        def _(s=s):
            ahalo_copy(s, s).wait_recv()
            ahalo_copy(s, 1 - s).wait_send()
    adj[:, 0] += ahalo[0]
    adj[:, rows - 1] += ahalo[1]
    send_row(1)
    inner = adjoint(3, rows - 4)
    for a in range(rows - 4):
        adj[:, 2 + a] = inner[a]

    def raised(x):
        hi, lo = split2(x)
        return split2(dot(hi, lv) + dot(lo, lv))

    def inside(k, carry):
        middle = field(k, 2, rows - 2).reshape(size - 4 * cols, levels)
        g = jnp.concatenate([gs[0, 1, k], gs[0, 0, k], middle, gs[1, 0, k], gs[1, 1, k]], axis=0)
        hi, lo = raised(g)
        back = dot(mm[...], hi) + dot(mm[...], lo)
        out[k] = alpha[k].astype(F32) + back.reshape(rows, cols, levels)
        return carry

    lax.fori_loop(0, members, inside, 0)

    for c in range(chunks):
        for s in range(2):
            @pl.when(has[s])
            def _(s=s, c=c):
                for w in range(2):
                    back_copy(s, s, w, c).wait_recv()

        def outer(k, carry):
            around = jnp.concatenate([gr[0, 0, k], gr[0, 1, k], gr[1, 1, k], gr[1, 0, k]], axis=0)
            hi, lo = raised(around)
            back = (dot(em[...], hi) + dot(em[...], lo)).reshape(4, cols, levels)
            out[k, 0:2] += back[0:2]
            out[k, rows - 2 : rows] += back[2:4]
            return carry

        lax.fori_loop(c * per, (c + 1) * per, outer, 0)
    for c in range(chunks):
        for s in range(2):
            @pl.when(has[s])
            def _(s=s, c=c):
                edge_copy(hs, hr, hs_sem, hr_sem, s, c).wait_send()
                for w in range(2):
                    back_copy(s, 1 - s, w, c).wait_send()


def solution(mesh):
    n = mesh.shape["mem"]
    tiles = mesh.shape["tile"]

    def on_device(alpha, ensemble, loc_vert, obs_col, obs_lev, obs_count, innovation, obs_weight):
        members, rows, cols, levels = alpha.shape
        slots = obs_col.shape[1]
        chunks = 4 if members % 4 == 0 else 1
        cq = cols // n
        vmem = pl.BlockSpec(memory_space=pltpu.VMEM)
        edge = pltpu.VMEM((2, members, 2, cols, levels), F32)
        turned = pltpu.VMEM((2, 2, members, cols, levels), F32)
        dma = pltpu.SemaphoreType.DMA
        return pl.pallas_call(
            functools.partial(kernel, n, tiles, chunks),
            out_shape=jax.ShapeDtypeStruct(alpha.shape, F32),
            in_specs=[vmem, pl.BlockSpec(memory_space=pl.ANY), vmem, vmem, vmem,
                      pl.BlockSpec(memory_space=pltpu.SMEM), vmem, vmem],
            out_specs=vmem,
            scratch_shapes=[
                pltpu.VMEM(ensemble.shape, BF16), edge, edge, turned, turned,
                pltpu.VMEM((members, 4, cols, levels), F32),
                pltpu.VMEM((rows * cols, rows * cols), BF16),
                pltpu.VMEM((4 * cols, 4 * cols), BF16),
                pltpu.VMEM((V * (rows + 2) * cols, slots), BF16),
                pltpu.VMEM((V, rows - 4, cols, levels), F32),
                pltpu.VMEM((V, 4, cols, levels), F32),
                pltpu.VMEM((n - 1, V, rows - 4, cq, levels), F32),
                pltpu.VMEM((n - 1, V, 4, cq, levels), F32),
                pltpu.VMEM((V, rows - 4, cq, levels), F32),
                pltpu.VMEM((V, 4, cq, levels), F32),
                pltpu.VMEM((V, rows - 4, cols, levels), F32),
                pltpu.VMEM((V, 4, cols, levels), F32),
                pltpu.VMEM((2, V, cols, levels), F32),
                pltpu.VMEM((V, rows, cols, levels), F32),
                pltpu.VMEM((2, V, cols, levels), F32),
                pltpu.VMEM((2, V, cols, levels), F32),
                dma, dma((2, chunks)), dma((2, chunks)), dma((2, 2, chunks)), dma((2, 2, chunks)),
                dma((2, n - 1)), dma((2, n - 1)), dma((2, n - 1)), dma((2, n - 1)),
                dma((2, n)), dma((2, n)), dma((2,)), dma((2,)),
            ],
            compiler_params=pltpu.CompilerParams(
                collective_id=0, has_side_effects=True, vmem_limit_bytes=50 << 20),
        )(alpha, ensemble, loc_vert, obs_col, obs_lev, obs_count, innovation, obs_weight)

    in_specs = (
        P("mem", "tile", None, None),
        P("mem", None, "tile", None, None),
        P(),
        P("tile", None),
        P("tile", None),
        P("tile"),
        P("tile", None),
        P("tile", None),
    )
    out_specs = P("mem", "tile", None, None)
    return jax.shard_map(
        on_device, mesh=mesh, in_specs=in_specs, out_specs=out_specs, check_vma=False
    )
```
